8 devices in a mesh: dp: 2 (over y, z), sp: 4 (over x, core).
Axes of the slice: x: 2, y: 2, z: 1, core: 2. Of those that a mesh axis runs over, the one named last changes fastest.
Arguments:
- q: bfloat16 [64, 48, 128], P('dp'), parts along dimension 0
- k: bfloat16 [64, 8192, 8, 128], P('dp', 'sp'), parts along dimension 0
- v: bfloat16 [64, 8192, 8, 128], P('dp', 'sp'), parts along dimension 0
Outputs:
- q: bfloat16 [64, 48, 128], P('dp'), parts along dimension 0
There are 2 independent parts. The reference program is written for one: setup_inputs(seed, part) draws one part's arguments, and reference() takes and returns one part's arrays. A program takes and returns all parts, laid end to end along the dimension named above; each array names one.
All inputs are finite; a program needn't handle non-finite values.
Results may differ from the reference program's by a relative error of at most 0.012.
Values are sent between devices in bfloat16 or wider.
A program may use at most 2 GiB of HBM per device.

```python
import jax
import jax.numpy as jnp

BATCH = 32
CACHE = 8192
HEADS = 48
KV_HEADS = 8
HEAD = 128


def setup_inputs(seed: int = 0, part: int = 0) -> dict:
    kq, kk, kv = (jax.random.fold_in(k, part) for k in jax.random.split(jax.random.key(seed), 3))
    return {
        "q": (3 * jax.random.normal(kq, (BATCH, HEADS, HEAD), jnp.float32)).astype(jnp.bfloat16),
        "k": jax.random.normal(kk, (BATCH, CACHE, KV_HEADS, HEAD), jnp.float32).astype(jnp.bfloat16),
        "v": jax.random.normal(kv, (BATCH, CACHE, KV_HEADS, HEAD), jnp.float32).astype(jnp.bfloat16),
    }


def einsum(form, a, b):
    return jnp.einsum(form, a.astype(jnp.float32), b.astype(jnp.float32))


def reference(q, k, v):
    grouped = q.reshape(BATCH, KV_HEADS, -1, HEAD)
    scores = einsum("bgsd,bugd->bgsu", grouped, k) * HEAD**-0.5
    weights = jax.nn.softmax(scores, -1).astype(jnp.bfloat16)
    return einsum("bgsu,bugd->bgsd", weights, v).astype(jnp.bfloat16).reshape(BATCH, HEADS, HEAD)
```

```python
import functools

import jax
import jax.numpy as jnp
from jax import lax
from jax.experimental import pallas as pl
from jax.experimental.pallas import tpu as pltpu
from jax.sharding import PartitionSpec as P

SLOTS = 3
LAG = 3
ROWS = 512
HALF = ROWS // 2
LOG2E = 1.4426950408889634


def iota(shape, axis):
    return lax.broadcasted_iota(jnp.int32, shape, axis)


def order(shape, axis):
    r = iota(shape, axis)
    j = r >> 3
    return (((r & 7) + j) & 7) * 6 + j


def kernel(
    devices, scale, q_ref, k_hbm, v_hbm, out_ref, kbuf, vbuf, sbuf, hbuf, qp, seen, stats, ksem, vsem, osend, ssend, orecv, srecv
):
    batch, queries, head = q_ref.shape
    members = queries // 8
    rows = k_hbm.shape[1]
    steps = rows // ROWS
    me = lax.axis_index("sp")

    def fetch_k(b):
        return pltpu.make_async_copy(k_hbm.at[b], kbuf.at[lax.rem(b, SLOTS)], ksem.at[lax.rem(b, SLOTS)])

    def fetch_v(b):
        return pltpu.make_async_copy(v_hbm.at[b], vbuf.at[lax.rem(b, SLOTS)], vsem.at[lax.rem(b, SLOTS)])

    for b in range(SLOTS):
        fetch_k(b).start()
        fetch_v(b).start()

    barrier = pltpu.get_barrier_semaphore()
    for hop in range(1, devices):
        pl.semaphore_signal(barrier, inc=1, device_id={"sp": lax.rem(me + hop, devices)})
    pl.semaphore_wait(barrier, devices - 1)

    def sends(b):
        copies = []
        for hop in range(1, devices):
            peer = {"sp": lax.rem(me + hop, devices)}
            copies.append(
                pltpu.make_async_remote_copy(
                    seen.at[me, b], seen.at[me, b], osend.at[hop - 1, lax.rem(b, 2)], orecv.at[hop - 1, b], device_id=peer
                )
            )
            copies.append(
                pltpu.make_async_remote_copy(
                    stats.at[me, b], stats.at[me, b], ssend.at[hop - 1, lax.rem(b, 2)], srecv.at[hop - 1, b], device_id=peer
                )
            )
        return copies

    def masks(lanes):
        return [((iota((8, lanes), 0) + j) & 7) == (iota((8, lanes), 1) & 7) for j in range(members)]

    def roll_all(x, op):
        for shift in (8, 16, 32, 64):
            x = op(x, pltpu.roll(x, shift, 1))
        return x

    pick = jnp.where(order((queries, queries), 0) == iota((queries, queries), 1), 1.0, 0.0).astype(jnp.bfloat16)

    def permute(b, _):
        qp[b] = jnp.dot(pick, q_ref[b], preferred_element_type=jnp.float32).astype(jnp.bfloat16)
        return 0

    lax.fori_loop(0, batch, permute, 0)

    def query_block(b):
        q = qp[b]
        zero = jnp.zeros_like(q)
        return jnp.concatenate([jnp.concatenate([q, zero], 1), jnp.concatenate([zero, q], 1)], 0)

    def scores_step(qb, sel, slot, t, b2, high):
        r = t * ROWS
        k2 = jnp.concatenate([kbuf[slot, pl.ds(r, HALF), :], kbuf[slot, pl.ds(r + HALF, HALF), :]], 1)
        s = lax.dot_general(qb, k2, (((1,), (1,)), ((), ())), preferred_element_type=jnp.float32)
        for half in range(2):
            base = half * queries
            x = s[base : base + 8]
            for j in range(1, members):
                x = jnp.where(sel[j], s[base + 8 * j : base + 8 * j + 8], x)
            sbuf[b2, :, pl.ds(r + half * HALF, HALF)] = x
            for c in range(0, HALF, 128):
                high = jnp.maximum(high, x[:, c : c + 128])
        return high

    def weights_step(spread, slot, t, b2, top, total):
        r = t * ROWS
        blocks = []
        for half in range(2):
            x = sbuf[b2, :, pl.ds(r + half * HALF, HALF)]
            w = jnp.exp2(x * scale - jnp.concatenate([top] * (HALF // 128), 1))
            for c in range(0, HALF, 128):
                total = total + w[:, c : c + 128]
            w16 = jnp.concatenate([w, w], 0).astype(jnp.bfloat16)
            blocks += [w16 * m for m in spread]
        v2 = jnp.concatenate([vbuf[slot, pl.ds(r, HALF), :], vbuf[slot, pl.ds(r + HALF, HALF), :]], 1)
        return jnp.dot(jnp.concatenate(blocks, 0), v2, preferred_element_type=jnp.float32), total

    def start_high():
        return jnp.full((8, 128), -jnp.inf, jnp.float32)

    def spreads():
        m = [jnp.where(x, 1.0, 0.0) for x in masks(HALF)]
        return [jnp.concatenate([m[2 * j], m[2 * j + 1]], 0).astype(jnp.bfloat16) for j in range(members // 2)]

    def finish(b, acc, total, top):
        o = acc[:queries, :head] + acc[queries:, head:]
        seen[me, b] = o.astype(jnp.bfloat16)
        stats[me, b] = jnp.where(iota((8, 128), 1) < 64, top, roll_all(total, jnp.add))

    def body(b, last):
        slot_v = lax.rem(b, SLOTS)
        now, later = lax.rem(b, 2), lax.rem(b + 1, 2)
        top = roll_all(hbuf[now], jnp.maximum) * scale
        spread = spreads()
        acc = None
        total = jnp.zeros((8, 128), jnp.float32)
        if not last:
            slot_k = lax.rem(b + 1, SLOTS)
            sel = masks(HALF)
            qb = query_block(b + 1)
            high = start_high()
        for t in range(steps):
            if not last:
                high = scores_step(qb, sel, slot_k, t, later, high)
            part, total = weights_step(spread, slot_v, t, now, top, total)
            acc = part if acc is None else acc + part
        if not last:
            hbuf[later] = high
        finish(b, acc, total, top)

    unpick = jnp.where(order((queries, queries), 1) == iota((queries, queries), 0), 1.0, 0.0).astype(jnp.bfloat16)

    def combine(b):
        for hop in range(1, devices):
            src = lax.rem(me + devices - hop, devices)
            pltpu.make_async_copy(seen.at[src, b], seen.at[src, b], orecv.at[hop - 1, b]).wait()
            pltpu.make_async_copy(stats.at[src, b], stats.at[src, b], srecv.at[hop - 1, b]).wait()
        tiles = [stats[d, b] for d in range(devices)]
        top = functools.reduce(jnp.maximum, tiles)
        ratio = [jnp.exp2(x - top) for x in tiles]
        whole = functools.reduce(jnp.add, [pltpu.roll(x, 64, 1) * e for x, e in zip(tiles, ratio)])
        ratio = [e / whole for e in ratio]
        out = []
        o = [seen[d, b].astype(jnp.float32) for d in range(devices)]
        for j in range(members):
            lane = (iota((8, 128), 0) + j) & 7
            rows_j = [
                x[8 * j : 8 * j + 8] * jnp.take_along_axis(e, lane, axis=1, mode="promise_in_bounds") for x, e in zip(o, ratio)
            ]
            out.append(functools.reduce(jnp.add, rows_j))
        mixed = jnp.concatenate(out, 0).astype(jnp.bfloat16)
        out_ref[b] = jnp.dot(unpick, mixed, preferred_element_type=jnp.float32).astype(jnp.bfloat16)

    fetch_k(0).wait()
    sel = masks(HALF)
    qb = query_block(0)
    high = start_high()
    for t in range(steps):
        high = scores_step(qb, sel, 0, t, 0, high)
    hbuf[0] = high

    def loop(b, _):
        fetch_k(b + 1).wait()
        fetch_v(b).wait()

        @pl.when(b + SLOTS < batch)
        def _():
            fetch_k(b + SLOTS).start()

        @pl.when((b >= 1) & (b - 1 + SLOTS < batch))
        def _():
            fetch_v(b - 1 + SLOTS).start()

        @pl.when(b >= 1)
        def _():
            @pl.when(b >= 3)
            def _():
                for c in sends(b - 3):
                    c.wait_send()

            for c in sends(b - 1):
                c.start()

        body(b, False)

        @pl.when(b >= LAG)
        def _():
            combine(b - LAG)

        return 0

    lax.fori_loop(0, batch - 1, loop, 0)

    last = batch - 1
    for c in sends(last - 3):
        c.wait_send()
    for c in sends(last - 1):
        c.start()
    fetch_v(last).wait()
    body(last, True)
    for c in sends(last - 2):
        c.wait_send()
    for c in sends(last):
        c.start()
    for b in range(batch - 1 - LAG, batch):
        combine(b)
    for b in (last - 1, last):
        for c in sends(b):
            c.wait_send()


def attend(mesh, q, k, v):
    batch, tokens, heads, head = k.shape
    devices = mesh.shape["sp"]
    queries = q.shape[1]
    rows = tokens * heads
    bf16, f32 = jnp.bfloat16, jnp.float32
    any_space = pl.BlockSpec(memory_space=pl.ANY)
    vmem = pl.BlockSpec(memory_space=pltpu.VMEM)
    return pl.pallas_call(
        functools.partial(kernel, devices, head**-0.5 * LOG2E),
        out_shape=jax.ShapeDtypeStruct(q.shape, bf16),
        in_specs=[vmem, any_space, any_space],
        out_specs=vmem,
        scratch_shapes=[
            pltpu.VMEM((SLOTS, rows, head), bf16),
            pltpu.VMEM((SLOTS, rows, head), bf16),
            pltpu.VMEM((2, 8, rows), f32),
            pltpu.VMEM((2, 8, 128), f32),
            pltpu.VMEM((batch, queries, head), bf16),
            pltpu.VMEM((devices, batch, queries, head), bf16),
            pltpu.VMEM((devices, batch, 8, 128), f32),
            pltpu.SemaphoreType.DMA((SLOTS,)),
            pltpu.SemaphoreType.DMA((SLOTS,)),
            pltpu.SemaphoreType.DMA((devices - 1, 2)),
            pltpu.SemaphoreType.DMA((devices - 1, 2)),
            pltpu.SemaphoreType.DMA((devices - 1, batch)),
            pltpu.SemaphoreType.DMA((devices - 1, batch)),
        ],
        compiler_params=pltpu.CompilerParams(collective_id=0, has_side_effects=True, vmem_limit_bytes=60 * 2**20),
        cost_estimate=pl.CostEstimate(flops=8 * 4 * q.size * tokens, bytes_accessed=2 * 2 * k.size, transcendentals=q.shape[0] * queries * tokens),
    )(q, k.reshape(batch, rows, head), v.reshape(batch, rows, head))


def solution(mesh):
    return jax.shard_map(
        functools.partial(attend, mesh),
        mesh=mesh,
        in_specs=(P("dp", None, None), P("dp", "sp", None, None), P("dp", "sp", None, None)),
        out_specs=P("dp", None, None),
        check_vma=False,
    )
```

```python
import functools

import jax
import jax.numpy as jnp
from jax import lax
from jax.experimental import pallas as pl
from jax.experimental.pallas import tpu as pltpu
from jax.sharding import PartitionSpec as P

SLOTS = 5
GROUP = 8
ROWS = 512
HALF = ROWS // 2
LOG2E = 1.4426950408889634


def iota(shape, axis):
    return lax.broadcasted_iota(jnp.int32, shape, axis)


def order(shape, axis):
    r = iota(shape, axis)
    j = r >> 3
    return (((r & 7) + j) & 7) * 6 + j


def kernel(
    devices, scale, q_ref, k_hbm, v_hbm, out_ref, kbuf, vbuf, sbuf, hbuf, acc_ref, sums, qp, seen, stats, parts, numbers, ksem, vsem,
    osend, ssend, orecv, srecv, rsend, rrecv, lsend, tsend, lrecv, trecv,
):
    batch, queries, head = q_ref.shape
    members = queries // 8
    rows = k_hbm.shape[1]
    steps = rows // ROWS
    groups = batch // devices - 1
    me = lax.axis_index("sp")

    def fetch_k(b):
        return pltpu.make_async_copy(k_hbm.at[b], kbuf.at[lax.rem(b, SLOTS)], ksem.at[lax.rem(b, SLOTS)])

    def fetch_v(b):
        return pltpu.make_async_copy(v_hbm.at[b], vbuf.at[lax.rem(b, SLOTS)], vsem.at[lax.rem(b, SLOTS)])

    for b in range(SLOTS):
        fetch_k(b).start()
        fetch_v(b).start()

    barrier = pltpu.get_barrier_semaphore()
    for hop in range(1, devices):
        pl.semaphore_signal(barrier, inc=1, device_id={"sp": lax.rem(me + hop, devices)})
    pl.semaphore_wait(barrier, devices - 1)

    def peer(hop):
        return {"sp": lax.rem(me + hop, devices)}

    def behind(hop):
        return lax.rem(me + devices - hop, devices)

    def remote(src, dst, send, recv, hop):
        return pltpu.make_async_remote_copy(src, dst, send, recv, device_id=peer(hop))

    def group_sends(g):
        copies = []
        for hop in range(1, devices):
            b = g * devices + lax.rem(me + hop, devices)
            n = hop - 1
            copies.append(remote(seen.at[b], parts.at[n, g], osend.at[n], orecv.at[n, g], hop))
            copies.append(remote(stats.at[b], numbers.at[n, g], ssend.at[n], srecv.at[n, g], hop))
        return copies

    def result_sends(g):
        at = out_ref.at[g * devices + me]
        return [remote(at, at, rsend.at[hop - 1], rrecv.at[hop - 1, g], hop) for hop in range(1, devices)]

    def last_sends(n):
        b = batch - devices + n
        copies = []
        for hop in range(1, devices):
            m = hop - 1
            copies.append(remote(seen.at[b], parts.at[m, groups + n], lsend.at[m, n], lrecv.at[m, n], hop))
            copies.append(remote(stats.at[b], numbers.at[m, groups + n], tsend.at[m, n], trecv.at[m, n], hop))
        return copies

    def masks(lanes):
        return [((iota((8, lanes), 0) + j) & 7) == (iota((8, lanes), 1) & 7) for j in range(members)]

    def roll_all(x, op):
        for shift in (8, 16, 32, 64):
            x = op(x, pltpu.roll(x, shift, 1))
        return x

    pick = jnp.where(order((queries, queries), 0) == iota((queries, queries), 1), 1.0, 0.0).astype(jnp.bfloat16)

    def permute(n, _):
        for b in range(8):
            b += n * 8
            qp[b] = jnp.dot(pick, q_ref[b], preferred_element_type=jnp.float32).astype(jnp.bfloat16)
        return 0

    lax.fori_loop(0, batch // 8, permute, 0)

    def query_block(b):
        q = qp[b]
        zero = jnp.zeros_like(q)
        return jnp.concatenate([jnp.concatenate([q, zero], 1), jnp.concatenate([zero, q], 1)], 0)

    def scores_step(qb, sel, slot, t, b2, high):
        r = t * ROWS
        k2 = jnp.concatenate([kbuf[slot, pl.ds(r, HALF), :], kbuf[slot, pl.ds(r + HALF, HALF), :]], 1)
        s = lax.dot_general(qb, k2, (((1,), (1,)), ((), ())), preferred_element_type=jnp.float32)
        for half in range(2):
            base = half * queries
            x = s[base : base + 8]
            for j in range(1, members):
                x = jnp.where(sel[j], s[base + 8 * j : base + 8 * j + 8], x)
            sbuf[b2, :, pl.ds(r + half * HALF, HALF)] = x
            for c in range(0, HALF, 128):
                high = jnp.maximum(high, x[:, c : c + 128])
        return high

    def weights_step(spread, slot, t, b2, top, total, acc):
        r = t * ROWS
        for half in range(2):
            at = pl.ds(r + half * HALF, HALF)
            w = jnp.exp2(sbuf[b2, :, at] * scale - jnp.concatenate([top] * (HALF // 128), 1))
            for c in range(0, HALF, 128):
                total = total + w[:, c : c + 128]
            w16 = jnp.concatenate([w, w], 0).astype(jnp.bfloat16)
            part = jnp.dot(
                jnp.concatenate([w16 * m for m in spread], 0), vbuf[slot, at, :], preferred_element_type=jnp.float32
            )
            acc = part if acc is None else acc + part
        return total, acc

    def start_high():
        return jnp.full((8, 128), -jnp.inf, jnp.float32)

    def spreads():
        m = [jnp.where(x, 1.0, 0.0) for x in masks(HALF)]
        return [jnp.concatenate([m[2 * j], m[2 * j + 1]], 0).astype(jnp.bfloat16) for j in range(members // 2)]

    def finish(b):
        seen[b] = acc_ref[...].astype(jnp.bfloat16)
        top, total = (pltpu.roll(x, 0, 1, stride=7, stride_axis=0) for x in (sums[0], roll_all(sums[1], jnp.add)))
        stats[b] = jnp.where(iota((8, 128), 1) < 64, top, total)

    def body(b, last):
        slot_v = lax.rem(b, SLOTS)
        now, later = lax.rem(b, 2), lax.rem(b + 1, 2)
        top = roll_all(hbuf[now], jnp.maximum) * scale
        spread = spreads()
        acc = None
        total = jnp.zeros((8, 128), jnp.float32)
        if not last:
            slot_k = lax.rem(b + 1, SLOTS)
            sel = masks(HALF)
            qb = query_block(b + 1)
            high = start_high()
        for g in range(0, steps, GROUP):
            if not last:
                for t in range(g, g + GROUP):
                    high = scores_step(qb, sel, slot_k, t, later, high)
            for t in range(g, g + GROUP):
                total, acc = weights_step(spread, slot_v, t, now, top, total, acc)
        if not last:
            hbuf[later] = high
        acc_ref[...] = acc
        sums[0] = top
        sums[1] = total

    unpick = jnp.where(order((queries, queries), 1) == iota((queries, queries), 0), 1.0, 0.0).astype(jnp.bfloat16)

    def combine(b, at):
        tiles, seens = [], []
        for d in range(devices):
            hop = lax.rem(me + devices - d, devices)
            far = jnp.maximum(hop - 1, 0)
            own = hop == 0
            tiles.append(jnp.where(own, stats[b], numbers[far, at]))
            seens.append(jnp.where(own, seen[b], parts[far, at]).astype(jnp.float32))
        top = functools.reduce(jnp.maximum, tiles)
        ratio = [jnp.exp2(x - top) for x in tiles]
        whole = functools.reduce(jnp.add, [pltpu.roll(x, 64, 1) * e for x, e in zip(tiles, ratio)])
        ratio = [e / whole for e in ratio]
        out = []
        for j in range(members):
            terms = [x[8 * j : 8 * j + 8] * jnp.broadcast_to(e[:, j : j + 1], (8, head)) for x, e in zip(seens, ratio)]
            out.append(functools.reduce(jnp.add, terms))
        mixed = jnp.concatenate(out, 0).astype(jnp.bfloat16)
        out_ref[b] = jnp.dot(unpick, mixed, preferred_element_type=jnp.float32).astype(jnp.bfloat16)

    def wait_recv(copies):
        for c in copies:
            c.wait_recv()

    def wait_send(copies):
        for c in copies:
            c.wait_send()

    def start(copies):
        for c in copies:
            c.start()

    def tick(t):
        @pl.when(t >= 1)
        def _():
            wait_send(group_sends(t - 1))

        @pl.when(t < groups)
        def _():
            start(group_sends(t))

        @pl.when(t >= 3)
        def _():
            wait_send(result_sends(t - 3))

        @pl.when(t >= 2)
        def _():
            start(result_sends(t - 2))

        @pl.when(t >= 1)
        def _():
            wait_recv(group_sends(t - 1))
            combine((t - 1) * devices + me, t - 1)

    acc_ref[...] = jnp.zeros_like(acc_ref)
    sums[...] = jnp.zeros_like(sums)

    fetch_k(0).wait()
    sel = masks(HALF)
    qb = query_block(0)
    high = start_high()
    for t in range(steps):
        high = scores_step(qb, sel, 0, t, 0, high)
    hbuf[0] = high

    def step(b):
        fetch_k(b + 1).wait()
        fetch_v(b).wait()

        @pl.when(b + SLOTS < batch)
        def _():
            fetch_k(b + SLOTS).start()

        @pl.when((b >= 1) & (b - 1 + SLOTS < batch))
        def _():
            fetch_v(b - 1 + SLOTS).start()

        finish(jnp.maximum(b - 1, 0))
        body(b, False)

    def loop(b, _):
        step(b)

        @pl.when((b >= devices) & (lax.rem(b, devices) == 0))
        def _():
            tick(lax.div(b, devices) - 1)

        return 0

    last = batch - 1
    lax.fori_loop(0, last - 2, loop, 0)
    step(last - 2)
    start(last_sends(0))
    step(last - 1)
    start(last_sends(1))
    tick(groups)
    finish(last - 1)
    fetch_v(last).wait()
    start(last_sends(2))
    body(last, True)
    finish(last)
    start(last_sends(3))
    wait_send(result_sends(groups - 2))
    start(result_sends(groups - 1))
    for n in range(devices):
        wait_recv(last_sends(n))
        combine(batch - devices + n, groups + n)
    for g in range(groups):
        wait_recv(result_sends(g))
    wait_send(result_sends(groups - 1))
    for n in range(devices):
        wait_send(last_sends(n))


def attend(mesh, q, k, v):
    batch, tokens, heads, head = k.shape
    devices = mesh.shape["sp"]
    queries = q.shape[1]
    rows = tokens * heads
    peers, groups, dma = devices - 1, batch // devices - 1, pltpu.SemaphoreType.DMA
    bf16, f32 = jnp.bfloat16, jnp.float32
    any_space = pl.BlockSpec(memory_space=pl.ANY)
    vmem = pl.BlockSpec(memory_space=pltpu.VMEM)
    return pl.pallas_call(
        functools.partial(kernel, devices, head**-0.5 * LOG2E),
        out_shape=jax.ShapeDtypeStruct(q.shape, bf16),
        in_specs=[vmem, any_space, any_space],
        out_specs=vmem,
        scratch_shapes=[
            pltpu.VMEM((SLOTS, rows, head), bf16),
            pltpu.VMEM((SLOTS, rows, head), bf16),
            pltpu.VMEM((2, 8, rows), f32),
            pltpu.VMEM((2, 8, 128), f32),
            pltpu.VMEM((queries, head), f32),
            pltpu.VMEM((2, 8, 128), f32),
            pltpu.VMEM((batch, queries, head), bf16),
            pltpu.VMEM((batch, queries, head), bf16),
            pltpu.VMEM((batch, 8, 128), f32),
            pltpu.VMEM((peers, groups + devices, queries, head), bf16),
            pltpu.VMEM((peers, groups + devices, 8, 128), f32),
            dma((SLOTS,)),
            dma((SLOTS,)),
            dma((peers,)),
            dma((peers,)),
            dma((peers, groups)),
            dma((peers, groups)),
            dma((peers,)),
            dma((peers, groups)),
            *[dma((peers, devices))] * 4,
        ],
        compiler_params=pltpu.CompilerParams(collective_id=0, has_side_effects=True, vmem_limit_bytes=60 * 2**20),
        cost_estimate=pl.CostEstimate(flops=8 * 4 * q.size * tokens, bytes_accessed=2 * 2 * k.size, transcendentals=q.shape[0] * queries * tokens),
    )(q, k.reshape(batch, rows, head), v.reshape(batch, rows, head))


def solution(mesh):
    return jax.shard_map(
        functools.partial(attend, mesh),
        mesh=mesh,
        in_specs=(P("dp", None, None), P("dp", "sp", None, None), P("dp", "sp", None, None)),
        out_specs=P("dp", None, None),
        check_vma=False,
    )
```

```python
import functools

import jax
import jax.numpy as jnp
from jax import lax
from jax.experimental import pallas as pl
from jax.experimental.pallas import tpu as pltpu
from jax.sharding import PartitionSpec as P

SLOTS = 5
GROUP = 8
ROWS = 512
HALF = ROWS // 2
LOG2E = 1.4426950408889634


def iota(shape, axis):
    return lax.broadcasted_iota(jnp.int32, shape, axis)


def order(shape, axis):
    r = iota(shape, axis)
    j = r >> 3
    return (((r & 7) + j) & 7) * 6 + j


def kernel(
    devices, scale, q_hbm, k_hbm, v_hbm, out_ref, q_ref, kbuf, vbuf, sbuf, hbuf, acc_ref, sums, qp, seen, stats, parts, numbers, qsem, ksem, vsem, psem,
    osend, ssend, orecv, srecv, rsend, rrecv, lsend, tsend, lrecv, trecv,
):
    batch, queries, head = q_hbm.shape
    members = queries // 8
    rows = k_hbm.shape[1]
    steps = rows // ROWS
    groups = batch // devices - 1
    last = batch - 1
    me = lax.axis_index("sp")

    def fetch_k(b):
        return pltpu.make_async_copy(k_hbm.at[b], kbuf.at[lax.rem(b, SLOTS)], ksem.at[lax.rem(b, SLOTS)])

    def fetch_v(b):
        return pltpu.make_async_copy(v_hbm.at[b], vbuf.at[lax.rem(b, SLOTS)], vsem.at[lax.rem(b, SLOTS)])

    fetch_q = pltpu.make_async_copy(q_hbm, q_ref, qsem)
    fetch_q.start()
    def fetch_piece(n):
        at = pl.ds(n * GROUP * ROWS, GROUP * ROWS)
        return pltpu.make_async_copy(v_hbm.at[last, at], vbuf.at[last % SLOTS, at], psem.at[n])

    fetch_k(0).start()
    fetch_k(1).start()
    fetch_v(0).start()

    barrier = pltpu.get_barrier_semaphore()
    for hop in range(1, devices):
        pl.semaphore_signal(barrier, inc=1, device_id={"sp": lax.rem(me + hop, devices)})
    pl.semaphore_wait(barrier, devices - 1)

    def peer(hop):
        return {"sp": lax.rem(me + hop, devices)}

    def behind(hop):
        return lax.rem(me + devices - hop, devices)

    def remote(src, dst, send, recv, hop):
        return pltpu.make_async_remote_copy(src, dst, send, recv, device_id=peer(hop))

    def group_sends(g):
        copies = []
        for hop in range(1, devices):
            b = g * devices + lax.rem(me + hop, devices)
            n = hop - 1
            copies.append(remote(seen.at[b], parts.at[n, g], osend.at[n], orecv.at[n, g], hop))
            copies.append(remote(stats.at[b], numbers.at[n, g], ssend.at[n], srecv.at[n, g], hop))
        return copies

    def result_sends(g):
        at = out_ref.at[g * devices + me]
        return [remote(at, at, rsend.at[hop - 1, lax.rem(g, 2)], rrecv.at[hop - 1, g], hop) for hop in range(1, devices)]

    def last_sends(n):
        b = batch - devices + n
        copies = []
        for hop in range(1, devices):
            m = hop - 1
            copies.append(remote(seen.at[b], parts.at[m, groups + n], lsend.at[m, n], lrecv.at[m, n], hop))
            copies.append(remote(stats.at[b], numbers.at[m, groups + n], tsend.at[m, n], trecv.at[m, n], hop))
        return copies

    def masks(lanes):
        return [((iota((8, lanes), 0) + j) & 7) == (iota((8, lanes), 1) & 7) for j in range(members)]

    def roll_all(x, op):
        for shift in (8, 16, 32, 64):
            x = op(x, pltpu.roll(x, shift, 1))
        return x

    pick = jnp.where(order((queries, queries), 0) == iota((queries, queries), 1), 1.0, 0.0).astype(jnp.bfloat16)

    def permute(n, _):
        for b in range(8):
            b += n * 8
            qp[b] = jnp.dot(pick, q_ref[b], preferred_element_type=jnp.float32).astype(jnp.bfloat16)
        return 0

    fetch_q.wait()
    lax.fori_loop(0, batch // 8, permute, 0)

    def query_block(b):
        q = qp[b]
        zero = jnp.zeros_like(q)
        return jnp.concatenate([jnp.concatenate([q, zero], 1), jnp.concatenate([zero, q], 1)], 0)

    def scores_step(qb, sel, slot, t, b2, high):
        r = t * ROWS
        k2 = jnp.concatenate([kbuf[slot, pl.ds(r, HALF), :], kbuf[slot, pl.ds(r + HALF, HALF), :]], 1)
        s = lax.dot_general(qb, k2, (((1,), (1,)), ((), ())), preferred_element_type=jnp.float32)
        for half in range(2):
            base = half * queries
            x = s[base : base + 8]
            for j in range(1, members):
                x = jnp.where(sel[j], s[base + 8 * j : base + 8 * j + 8], x)
            sbuf[b2, :, pl.ds(r + half * HALF, HALF)] = x
            for c in range(0, HALF, 128):
                high = jnp.maximum(high, x[:, c : c + 128])
        return high

    def weights_step(spread, slot, t, b2, top, total, acc):
        r = t * ROWS
        for half in range(2):
            at = pl.ds(r + half * HALF, HALF)
            w = jnp.exp2(sbuf[b2, :, at] * scale - jnp.concatenate([top] * (HALF // 128), 1))
            for c in range(0, HALF, 128):
                total = total + w[:, c : c + 128]
            w16 = jnp.concatenate([w, w], 0).astype(jnp.bfloat16)
            part = jnp.dot(
                jnp.concatenate([w16 * m for m in spread], 0), vbuf[slot, at, :], preferred_element_type=jnp.float32
            )
            acc = part if acc is None else acc + part
        return total, acc

    def start_high():
        return jnp.full((8, 128), -jnp.inf, jnp.float32)

    def spreads():
        m = [jnp.where(x, 1.0, 0.0) for x in masks(HALF)]
        return [jnp.concatenate([m[2 * j], m[2 * j + 1]], 0).astype(jnp.bfloat16) for j in range(members // 2)]

    def finish(b):
        seen[b] = acc_ref[...].astype(jnp.bfloat16)
        top, total = (pltpu.roll(x, 0, 1, stride=7, stride_axis=0) for x in (sums[0], roll_all(sums[1], jnp.add)))
        stats[b] = jnp.where(iota((8, 128), 1) < 64, top, total)

    def body(scores, weights, before=None):
        if weights is not None:
            slot_v, now = lax.rem(weights, SLOTS), lax.rem(weights, 2)
            top = roll_all(hbuf[now], jnp.maximum) * scale
            spread = spreads()
            acc = None
            total = jnp.zeros((8, 128), jnp.float32)
        if scores is not None:
            slot_k, later = lax.rem(scores, SLOTS), lax.rem(scores, 2)
            sel = masks(HALF)
            qb = query_block(scores)
            high = start_high()
        for g in range(steps // GROUP):
            if before is not None:
                before(g)
            if scores is not None:
                for t in range(g * GROUP, g * GROUP + GROUP):
                    high = scores_step(qb, sel, slot_k, t, later, high)
            if weights is not None:
                for t in range(g * GROUP, g * GROUP + GROUP):
                    total, acc = weights_step(spread, slot_v, t, now, top, total, acc)
        if scores is not None:
            hbuf[later] = high
        if weights is not None:
            acc_ref[...] = acc
            sums[0] = top
            sums[1] = total

    unpick = jnp.where(order((queries, queries), 1) == iota((queries, queries), 0), 1.0, 0.0).astype(jnp.bfloat16)

    def combine(b, at):
        tiles, seens = [], []
        for d in range(devices):
            hop = lax.rem(me + devices - d, devices)
            far = jnp.maximum(hop - 1, 0)
            own = hop == 0
            tiles.append(jnp.where(own, stats[b], numbers[far, at]))
            seens.append(jnp.where(own, seen[b], parts[far, at]).astype(jnp.float32))
        top = functools.reduce(jnp.maximum, tiles)
        ratio = [jnp.exp2(x - top) for x in tiles]
        whole = functools.reduce(jnp.add, [pltpu.roll(x, 64, 1) * e for x, e in zip(tiles, ratio)])
        ratio = [e / whole for e in ratio]
        out = []
        for j in range(members):
            terms = [x[8 * j : 8 * j + 8] * jnp.broadcast_to(e[:, j : j + 1], (8, head)) for x, e in zip(seens, ratio)]
            out.append(functools.reduce(jnp.add, terms))
        mixed = jnp.concatenate(out, 0).astype(jnp.bfloat16)
        out_ref[b] = jnp.dot(unpick, mixed, preferred_element_type=jnp.float32).astype(jnp.bfloat16)

    def wait_recv(copies):
        for c in copies:
            c.wait_recv()

    def wait_send(copies):
        for c in copies:
            c.wait_send()

    def start(copies):
        for c in copies:
            c.start()

    def tick(t):
        @pl.when(t >= 1)
        def _():
            wait_send(group_sends(t - 1))

        @pl.when(t < groups)
        def _():
            start(group_sends(t))

        @pl.when(t >= 4)
        def _():
            wait_send(result_sends(t - 4))

        @pl.when(t >= 2)
        def _():
            start(result_sends(t - 2))

        @pl.when(t >= 1)
        def _():
            wait_recv(group_sends(t - 1))
            combine((t - 1) * devices + me, t - 1)

    acc_ref[...] = jnp.zeros_like(acc_ref)
    sums[...] = jnp.zeros_like(sums)

    fetch_k(0).wait()
    for b in range(1, SLOTS - 1):
        fetch_k(b + 1).start()
        fetch_v(b).start()
    body(0, None)

    def step(b):
        fetch_k(b + 1).wait()
        fetch_v(b).wait()

        @pl.when(b + SLOTS < batch)
        def _():
            fetch_k(b + SLOTS).start()

        @pl.when(b - 1 + SLOTS < last)
        def _():
            fetch_v(b - 1 + SLOTS).start()

        @pl.when(b - 1 + SLOTS == last)
        def _():
            for n in range(steps // GROUP):
                fetch_piece(n).start()

        finish(jnp.maximum(b - 1, 0))
        body(b + 1, b)

    def loop(b, _):
        step(b)

        @pl.when((b >= devices) & (lax.rem(b, devices) == 0))
        def _():
            tick(lax.div(b, devices) - 1)

        return 0

    lax.fori_loop(0, last - 2, loop, 0)
    step(last - 2)
    start(last_sends(0))
    fetch_k(last).wait()
    finish(last - 2)
    body(last, None)
    start(last_sends(1))
    fetch_v(last - 1).wait()
    body(None, last - 1)
    finish(last - 1)
    start(last_sends(2))

    def before(g):
        fetch_piece(g).wait()

    body(None, last, before)
    finish(last)
    start(last_sends(3))
    tick(groups)
    wait_send(result_sends(groups - 3))
    start(result_sends(groups - 1))
    for n in range(devices):
        wait_recv(last_sends(n))
        combine(batch - devices + n, groups + n)
    for g in range(groups):
        wait_recv(result_sends(g))
    for g in range(groups - 2, groups):
        wait_send(result_sends(g))
    for n in range(devices):
        wait_send(last_sends(n))


def attend(mesh, q, k, v):
    batch, tokens, heads, head = k.shape
    devices = mesh.shape["sp"]
    queries = q.shape[1]
    rows = tokens * heads
    peers, groups, dma = devices - 1, batch // devices - 1, pltpu.SemaphoreType.DMA
    bf16, f32 = jnp.bfloat16, jnp.float32
    any_space = pl.BlockSpec(memory_space=pl.ANY)
    vmem = pl.BlockSpec(memory_space=pltpu.VMEM)
    return pl.pallas_call(
        functools.partial(kernel, devices, head**-0.5 * LOG2E),
        out_shape=pltpu.VMEM(q.shape, bf16),
        in_specs=[any_space] * 3,
        out_specs=vmem,
        scratch_shapes=[
            pltpu.VMEM(q.shape, bf16),
            pltpu.VMEM((SLOTS, rows, head), bf16),
            pltpu.VMEM((SLOTS, rows, head), bf16),
            pltpu.VMEM((2, 8, rows), f32),
            pltpu.VMEM((2, 8, 128), f32),
            pltpu.VMEM((queries, head), f32),
            pltpu.VMEM((2, 8, 128), f32),
            pltpu.VMEM((batch, queries, head), bf16),
            pltpu.VMEM((batch, queries, head), bf16),
            pltpu.VMEM((batch, 8, 128), f32),
            pltpu.VMEM((peers, groups + devices, queries, head), bf16),
            pltpu.VMEM((peers, groups + devices, 8, 128), f32),
            dma,
            dma((SLOTS,)),
            dma((SLOTS,)),
            dma((rows // (GROUP * ROWS),)),
            dma((peers,)),
            dma((peers,)),
            dma((peers, groups)),
            dma((peers, groups)),
            dma((peers, 2)),
            dma((peers, groups)),
            *[dma((peers, devices))] * 4,
        ],
        compiler_params=pltpu.CompilerParams(collective_id=0, has_side_effects=True, vmem_limit_bytes=60 * 2**20),
        cost_estimate=pl.CostEstimate(flops=8 * 4 * q.size * tokens, bytes_accessed=2 * 2 * k.size, transcendentals=q.shape[0] * queries * tokens),
    )(q, k.reshape(batch, rows, head), v.reshape(batch, rows, head))


def solution(mesh):
    return jax.shard_map(
        functools.partial(attend, mesh),
        mesh=mesh,
        in_specs=(P("dp", None, None), P("dp", "sp", None, None), P("dp", "sp", None, None)),
        out_specs=P("dp", None, None),
        check_vma=False,
    )
```

```python
import functools

import jax
import jax.numpy as jnp
from jax import lax
from jax.experimental import pallas as pl
from jax.experimental.pallas import tpu as pltpu
from jax.sharding import PartitionSpec as P

SLOTS = 5
GROUP = 8
ROWS = 512
HALF = ROWS // 2
LOG2E = 1.4426950408889634


def iota(shape, axis):
    return lax.broadcasted_iota(jnp.int32, shape, axis)


def order(shape, axis):
    r = iota(shape, axis)
    j = r >> 3
    return (((r & 7) + j) & 7) * 6 + j


def kernel(
    devices, scale, q_hbm, k_hbm, v_hbm, out_ref, q_ref, kbuf, vbuf, sbuf, hbuf, acc_ref, sums, qp, seen, stats, parts, numbers, qsem, ksem, vsem, psem,
    osend, ssend, orecv, srecv, rsend, rrecv, lsend, tsend, lrecv, trecv,
):
    batch, queries, head = q_hbm.shape
    members = queries // 8
    rows = k_hbm.shape[1]
    steps = rows // ROWS
    groups = batch // devices - 1
    last = batch - 1
    me = lax.axis_index("sp")

    def fetch_k(b):
        return pltpu.make_async_copy(k_hbm.at[b], kbuf.at[lax.rem(b, SLOTS)], ksem.at[lax.rem(b, SLOTS)])

    def fetch_v(b):
        return pltpu.make_async_copy(v_hbm.at[b], vbuf.at[lax.rem(b, SLOTS)], vsem.at[lax.rem(b, SLOTS)])

    fetch_q = pltpu.make_async_copy(q_hbm, q_ref, qsem)
    fetch_q.start()
    def fetch_piece(n):
        at = pl.ds(n * GROUP * ROWS, GROUP * ROWS)
        return pltpu.make_async_copy(v_hbm.at[last, at], vbuf.at[last % SLOTS, at], psem.at[n])

    fetch_k(0).start()
    fetch_k(1).start()
    fetch_v(0).start()

    barrier = pltpu.get_barrier_semaphore()
    for hop in range(1, devices):
        pl.semaphore_signal(barrier, inc=1, device_id={"sp": lax.rem(me + hop, devices)})
    pl.semaphore_wait(barrier, devices - 1)

    def peer(hop):
        return {"sp": lax.rem(me + hop, devices)}

    def behind(hop):
        return lax.rem(me + devices - hop, devices)

    def remote(src, dst, send, recv, hop):
        return pltpu.make_async_remote_copy(src, dst, send, recv, device_id=peer(hop))

    def group_sends(g):
        copies = []
        for hop in range(1, devices):
            b = g * devices + lax.rem(me + hop, devices)
            n = hop - 1
            copies.append(remote(seen.at[b], parts.at[n, g], osend.at[n], orecv.at[n, g], hop))
            copies.append(remote(stats.at[b], numbers.at[n, g], ssend.at[n], srecv.at[n, g], hop))
        return copies

    def result_sends(g):
        at = out_ref.at[g * devices + me]
        return [remote(at, at, rsend.at[hop - 1, lax.rem(g, 2)], rrecv.at[hop - 1, g], hop) for hop in range(1, devices)]

    def last_sends(n):
        b = batch - devices + n
        copies = []
        for hop in range(1, devices):
            m = hop - 1
            copies.append(remote(seen.at[b], parts.at[m, groups + n], lsend.at[m, n], lrecv.at[m, n], hop))
            copies.append(remote(stats.at[b], numbers.at[m, groups + n], tsend.at[m, n], trecv.at[m, n], hop))
        return copies

    def masks(lanes):
        return [((iota((8, lanes), 0) + j) & 7) == (iota((8, lanes), 1) & 7) for j in range(members)]

    def roll_all(x, op):
        for shift in (8, 16, 32, 64):
            x = op(x, pltpu.roll(x, shift, 1))
        return x

    pick = jnp.where(order((queries, queries), 0) == iota((queries, queries), 1), 1.0, 0.0).astype(jnp.bfloat16)

    def permute(n, _):
        for b in range(8):
            b += n * 8
            qp[b] = jnp.dot(pick, q_ref[b], preferred_element_type=jnp.float32).astype(jnp.bfloat16)
        return 0

    fetch_q.wait()
    lax.fori_loop(0, batch // 8, permute, 0)

    def query_block(b):
        q = qp[b]
        zero = jnp.zeros_like(q)
        return jnp.concatenate([jnp.concatenate([q, zero], 1), jnp.concatenate([zero, q], 1)], 0)

    def scores_step(qb, sel, slot, t, b2, high):
        r = t * ROWS
        k2 = jnp.concatenate([kbuf[slot, pl.ds(r, HALF), :], kbuf[slot, pl.ds(r + HALF, HALF), :]], 1)
        s = lax.dot_general(qb, k2, (((1,), (1,)), ((), ())), preferred_element_type=jnp.float32)
        for half in range(2):
            base = half * queries
            x = s[base : base + 8]
            for j in range(1, members):
                x = jnp.where(sel[j], s[base + 8 * j : base + 8 * j + 8], x)
            sbuf[b2, :, pl.ds(r + half * HALF, HALF)] = x
            for c in range(0, HALF, 128):
                high = jnp.maximum(high, x[:, c : c + 128])
        return high

    def weights_step(spread, slot, t, b2, top, total, acc):
        r = t * ROWS
        for half in range(2):
            at = pl.ds(r + half * HALF, HALF)
            w = jnp.exp2(sbuf[b2, :, at] * scale - jnp.concatenate([top] * (HALF // 128), 1))
            for c in range(0, HALF, 128):
                total = total + w[:, c : c + 128]
            w16 = jnp.concatenate([w, w], 0).astype(jnp.bfloat16)
            part = jnp.dot(
                jnp.concatenate([w16 * m for m in spread], 0), vbuf[slot, at, :], preferred_element_type=jnp.float32
            )
            acc = part if acc is None else acc + part
        return total, acc

    def start_high():
        return jnp.full((8, 128), -jnp.inf, jnp.float32)

    def spreads():
        m = [jnp.where(x, 1.0, 0.0) for x in masks(HALF)]
        return [jnp.concatenate([m[2 * j], m[2 * j + 1]], 0).astype(jnp.bfloat16) for j in range(members // 2)]

    def finish(b):
        finish_seen(b)
        finish_stats(b)

    def finish_seen(b):
        seen[b] = acc_ref[...].astype(jnp.bfloat16)

    def finish_stats(b):
        top, total = (pltpu.roll(x, 0, 1, stride=7, stride_axis=0) for x in (sums[0], roll_all(sums[1], jnp.add)))
        stats[b] = jnp.where(iota((8, 128), 1) < 64, top, total)

    def body(scores, weights, before=None):
        if weights is not None:
            slot_v, now = lax.rem(weights, SLOTS), lax.rem(weights, 2)
            top = roll_all(hbuf[now], jnp.maximum) * scale
            spread = spreads()
            acc = None
            total = jnp.zeros((8, 128), jnp.float32)
        if scores is not None:
            slot_k, later = lax.rem(scores, SLOTS), lax.rem(scores, 2)
            sel = masks(HALF)
            qb = query_block(scores)
            high = start_high()
        for g in range(steps // GROUP):
            if before is not None:
                before(g)
            if scores is not None:
                for t in range(g * GROUP, g * GROUP + GROUP):
                    high = scores_step(qb, sel, slot_k, t, later, high)
            if weights is not None:
                for t in range(g * GROUP, g * GROUP + GROUP):
                    total, acc = weights_step(spread, slot_v, t, now, top, total, acc)
        if scores is not None:
            hbuf[later] = high
        if weights is not None:
            acc_ref[...] = acc
            sums[0] = top
            sums[1] = total

    unpick = jnp.where(order((queries, queries), 1) == iota((queries, queries), 0), 1.0, 0.0).astype(jnp.bfloat16)

    def combine(b, at):
        tiles, seens = [], []
        for d in range(devices):
            hop = lax.rem(me + devices - d, devices)
            far = jnp.maximum(hop - 1, 0)
            own = hop == 0
            tiles.append(jnp.where(own, stats[b], numbers[far, at]))
            seens.append(jnp.where(own, seen[b], parts[far, at]).astype(jnp.float32))
        top = functools.reduce(jnp.maximum, tiles)
        ratio = [jnp.exp2(x - top) for x in tiles]
        whole = functools.reduce(jnp.add, [pltpu.roll(x, 64, 1) * e for x, e in zip(tiles, ratio)])
        ratio = [e / whole for e in ratio]
        out = []
        for j in range(members):
            terms = [x[8 * j : 8 * j + 8] * jnp.broadcast_to(e[:, j : j + 1], (8, head)) for x, e in zip(seens, ratio)]
            out.append(functools.reduce(jnp.add, terms))
        mixed = jnp.concatenate(out, 0).astype(jnp.bfloat16)
        out_ref[b] = jnp.dot(unpick, mixed, preferred_element_type=jnp.float32).astype(jnp.bfloat16)

    def wait_recv(copies):
        for c in copies:
            c.wait_recv()

    def wait_send(copies):
        for c in copies:
            c.wait_send()

    def start(copies):
        for c in copies:
            c.start()

    def tick(t):
        @pl.when(t >= 1)
        def _():
            wait_send(group_sends(t - 1))

        @pl.when(t < groups)
        def _():
            start(group_sends(t))

        @pl.when(t >= 4)
        def _():
            wait_send(result_sends(t - 4))

        @pl.when(t >= 2)
        def _():
            start(result_sends(t - 2))

        @pl.when(t >= 1)
        def _():
            wait_recv(group_sends(t - 1))
            combine((t - 1) * devices + me, t - 1)

    acc_ref[...] = jnp.zeros_like(acc_ref)
    sums[...] = jnp.zeros_like(sums)

    fetch_k(0).wait()
    for b in range(1, SLOTS - 1):
        fetch_k(b + 1).start()
        fetch_v(b).start()
    body(0, None)

    def step(b):
        fetch_k(b + 1).wait()
        fetch_v(b).wait()

        @pl.when(b + SLOTS < batch)
        def _():
            fetch_k(b + SLOTS).start()

        @pl.when(b - 1 + SLOTS < last)
        def _():
            fetch_v(b - 1 + SLOTS).start()

        @pl.when(b - 1 + SLOTS == last)
        def _():
            for n in range(steps // GROUP):
                fetch_piece(n).start()

        finish(jnp.maximum(b - 1, 0))
        body(b + 1, b)

    def loop(b, _):
        step(b)

        @pl.when((b >= devices) & (lax.rem(b, devices) == 0))
        def _():
            tick(lax.div(b, devices) - 1)

        return 0

    lax.fori_loop(0, last - 2, loop, 0)
    fetch_k(last - 1).wait()
    finish(last - 3)
    body(last - 1, None)
    start(last_sends(0))
    fetch_v(last - 2).wait()
    body(None, last - 2)
    fetch_k(last).wait()
    finish(last - 2)
    body(last, None)
    start(last_sends(1))
    fetch_v(last - 1).wait()
    body(None, last - 1)
    finish(last - 1)
    start(last_sends(2))

    pieces = steps // GROUP

    def before(g):
        for n in range(pieces - 1) if g == 0 else [g] if g == pieces - 1 else []:
            fetch_piece(n).wait()

    body(None, last, before)
    finish_seen(last)
    start(last_sends(devices - 1)[0::2])
    finish_stats(last)
    start(last_sends(devices - 1)[1::2])
    tick(groups)
    wait_send(result_sends(groups - 3))
    start(result_sends(groups - 1))
    for n in range(devices):
        wait_recv(last_sends(n))
        combine(batch - devices + n, groups + n)
    for g in range(groups):
        wait_recv(result_sends(g))
    for g in range(groups - 2, groups):
        wait_send(result_sends(g))
    for n in range(devices):
        wait_send(last_sends(n))


def attend(mesh, q, k, v):
    batch, tokens, heads, head = k.shape
    devices = mesh.shape["sp"]
    queries = q.shape[1]
    rows = tokens * heads
    peers, groups, dma = devices - 1, batch // devices - 1, pltpu.SemaphoreType.DMA
    bf16, f32 = jnp.bfloat16, jnp.float32
    any_space = pl.BlockSpec(memory_space=pl.ANY)
    vmem = pl.BlockSpec(memory_space=pltpu.VMEM)
    return pl.pallas_call(
        functools.partial(kernel, devices, head**-0.5 * LOG2E),
        out_shape=pltpu.VMEM(q.shape, bf16),
        in_specs=[any_space] * 3,
        out_specs=vmem,
        scratch_shapes=[
            pltpu.VMEM(q.shape, bf16),
            pltpu.VMEM((SLOTS, rows, head), bf16),
            pltpu.VMEM((SLOTS, rows, head), bf16),
            pltpu.VMEM((2, 8, rows), f32),
            pltpu.VMEM((2, 8, 128), f32),
            pltpu.VMEM((queries, head), f32),
            pltpu.VMEM((2, 8, 128), f32),
            pltpu.VMEM((batch, queries, head), bf16),
            pltpu.VMEM((batch, queries, head), bf16),
            pltpu.VMEM((batch, 8, 128), f32),
            pltpu.VMEM((peers, groups + devices, queries, head), bf16),
            pltpu.VMEM((peers, groups + devices, 8, 128), f32),
            dma,
            dma((SLOTS,)),
            dma((SLOTS,)),
            dma((rows // (GROUP * ROWS),)),
            dma((peers,)),
            dma((peers,)),
            dma((peers, groups)),
            dma((peers, groups)),
            dma((peers, 2)),
            dma((peers, groups)),
            *[dma((peers, devices))] * 4,
        ],
        compiler_params=pltpu.CompilerParams(collective_id=0, has_side_effects=True, vmem_limit_bytes=60 * 2**20),
        cost_estimate=pl.CostEstimate(flops=8 * 4 * q.size * tokens, bytes_accessed=2 * 2 * k.size, transcendentals=q.shape[0] * queries * tokens),
    )(q, k.reshape(batch, rows, head), v.reshape(batch, rows, head))


def solution(mesh):
    return jax.shard_map(
        functools.partial(attend, mesh),
        mesh=mesh,
        in_specs=(P("dp", None, None), P("dp", "sp", None, None), P("dp", "sp", None, None)),
        out_specs=P("dp", None, None),
        check_vma=False,
    )
```

```python
import functools

import jax
import jax.numpy as jnp
from jax import lax
from jax.experimental import pallas as pl
from jax.experimental.pallas import tpu as pltpu
from jax.sharding import PartitionSpec as P

SLOTS = 5
GROUP = 8
ROWS = 512
HALF = ROWS // 2
LOG2E = 1.4426950408889634


def iota(shape, axis):
    return lax.broadcasted_iota(jnp.int32, shape, axis)


def order(shape, axis):
    r = iota(shape, axis)
    j = r >> 3
    return (((r & 7) + j) & 7) * 6 + j


def kernel(
    devices, scale, q_hbm, k_hbm, v_hbm, out_ref, q_ref, kbuf, vbuf, sbuf, hbuf, acc_ref, sums, qp, seen, stats, parts, numbers, qsem, ksem, vsem, psem,
    osend, ssend, orecv, srecv, rsend, rrecv, lsend, tsend, lrecv, trecv,
):
    batch, queries, head = q_hbm.shape
    members = queries // 8
    rows = k_hbm.shape[1]
    steps = rows // ROWS
    groups = batch // devices - 1
    last = batch - 1
    me = lax.axis_index("sp")

    def fetch_k(b):
        return pltpu.make_async_copy(k_hbm.at[b], kbuf.at[lax.rem(b, SLOTS)], ksem.at[lax.rem(b, SLOTS)])

    def fetch_v(b):
        return pltpu.make_async_copy(v_hbm.at[b], vbuf.at[lax.rem(b, SLOTS)], vsem.at[lax.rem(b, SLOTS)])

    fetch_q = pltpu.make_async_copy(q_hbm, q_ref, qsem)
    fetch_q.start()
    def fetch_piece(n):
        at = pl.ds(n * GROUP * ROWS, GROUP * ROWS)
        return pltpu.make_async_copy(v_hbm.at[last, at], vbuf.at[last % SLOTS, at], psem.at[n])

    fetch_k(0).start()
    fetch_k(1).start()
    fetch_v(0).start()

    barrier = pltpu.get_barrier_semaphore()
    for hop in range(1, devices):
        pl.semaphore_signal(barrier, inc=1, device_id={"sp": lax.rem(me + hop, devices)})
    pl.semaphore_wait(barrier, devices - 1)

    def peer(hop):
        return {"sp": lax.rem(me + hop, devices)}

    def behind(hop):
        return lax.rem(me + devices - hop, devices)

    def remote(src, dst, send, recv, hop):
        return pltpu.make_async_remote_copy(src, dst, send, recv, device_id=peer(hop))

    def group_sends(g):
        copies = []
        for hop in range(1, devices):
            b = g * devices + lax.rem(me + hop, devices)
            n = hop - 1
            copies.append(remote(seen.at[b], parts.at[n, g], osend.at[n], orecv.at[n, g], hop))
            copies.append(remote(stats.at[b], numbers.at[n, g], ssend.at[n], srecv.at[n, g], hop))
        return copies

    def result_sends(g):
        at = out_ref.at[g * devices + me]
        return [remote(at, at, rsend.at[hop - 1, lax.rem(g, 2)], rrecv.at[hop - 1, g], hop) for hop in range(1, devices)]

    def last_sends(n):
        b = batch - devices + n
        copies = []
        for hop in range(1, devices):
            m = hop - 1
            copies.append(remote(seen.at[b], parts.at[m, groups + n], lsend.at[m, n], lrecv.at[m, n], hop))
            copies.append(remote(stats.at[b], numbers.at[m, groups + n], tsend.at[m, n], trecv.at[m, n], hop))
        return copies

    def masks(lanes):
        return [((iota((8, lanes), 0) + j) & 7) == (iota((8, lanes), 1) & 7) for j in range(members)]

    def roll_all(x, op):
        for shift in (8, 16, 32, 64):
            x = op(x, pltpu.roll(x, shift, 1))
        return x

    pick = jnp.where(order((queries, queries), 0) == iota((queries, queries), 1), 1.0, 0.0).astype(jnp.bfloat16)

    def permute(n, _):
        for b in range(8):
            b += n * 8
            qp[b] = jnp.dot(pick, q_ref[b], preferred_element_type=jnp.float32).astype(jnp.bfloat16)
        return 0

    fetch_q.wait()
    lax.fori_loop(0, batch // 8, permute, 0)

    def query_block(b):
        q = qp[b]
        zero = jnp.zeros_like(q)
        return jnp.concatenate([jnp.concatenate([q, zero], 1), jnp.concatenate([zero, q], 1)], 0)

    def scores_step(qb, sel, slot, t, b2, high):
        r = t * ROWS
        k2 = jnp.concatenate([kbuf[slot, pl.ds(r, HALF), :], kbuf[slot, pl.ds(r + HALF, HALF), :]], 1)
        s = lax.dot_general(qb, k2, (((1,), (1,)), ((), ())), preferred_element_type=jnp.float32)
        for half in range(2):
            base = half * queries
            x = jnp.zeros((8, HALF), jnp.float32)
            for j in range(members):
                x = jnp.where(sel[j], s[base + 8 * j : base + 8 * j + 8], x)
            sbuf[b2, :, pl.ds(r + half * HALF, HALF)] = x
            for c in range(0, HALF, 128):
                high = jnp.maximum(high, x[:, c : c + 128])
        return high

    def weights_step(spread, slot, t, b2, top, total, acc):
        r = t * ROWS
        for half in range(2):
            at = pl.ds(r + half * HALF, HALF)
            w = jnp.exp2(sbuf[b2, :, at] * scale - jnp.concatenate([top] * (HALF // 128), 1))
            for c in range(0, HALF, 128):
                total = total + w[:, c : c + 128]
            w16 = jnp.concatenate([w, w], 0).astype(jnp.bfloat16)
            part = jnp.dot(
                jnp.concatenate([w16 * m for m in spread], 0), vbuf[slot, at, :], preferred_element_type=jnp.float32
            )
            acc = part if acc is None else acc + part
        return total, acc

    def start_high():
        return jnp.full((8, 128), -jnp.inf, jnp.float32)

    def spreads():
        m = [jnp.where(x, 1.0, 0.0) for x in masks(HALF)]
        return [jnp.concatenate([m[2 * j], m[2 * j + 1]], 0).astype(jnp.bfloat16) for j in range(members // 2)]

    def finish(b):
        finish_seen(b)
        finish_stats(b)

    def finish_seen(b):
        seen[b] = acc_ref[...].astype(jnp.bfloat16)

    def finish_stats(b):
        top, total = (pltpu.roll(x, 0, 1, stride=7, stride_axis=0) for x in (sums[0], roll_all(sums[1], jnp.add)))
        stats[b] = jnp.where(iota((8, 128), 1) < 64, top, total)

    def body(scores, weights, before=None):
        if weights is not None:
            slot_v, now = lax.rem(weights, SLOTS), lax.rem(weights, 2)
            top = roll_all(hbuf[now], jnp.maximum) * scale
            spread = spreads()
            acc = None
            total = jnp.zeros((8, 128), jnp.float32)
        if scores is not None:
            slot_k, later = lax.rem(scores, SLOTS), lax.rem(scores, 2)
            sel = masks(HALF)
            qb = query_block(scores)
            high = start_high()
        for g in range(steps // GROUP):
            if before is not None:
                before(g)
            if scores is not None:
                for t in range(g * GROUP, g * GROUP + GROUP):
                    high = scores_step(qb, sel, slot_k, t, later, high)
            if weights is not None:
                for t in range(g * GROUP, g * GROUP + GROUP):
                    total, acc = weights_step(spread, slot_v, t, now, top, total, acc)
        if scores is not None:
            hbuf[later] = high
        if weights is not None:
            acc_ref[...] = acc
            sums[0] = top
            sums[1] = total

    unpick = jnp.where(order((queries, queries), 1) == iota((queries, queries), 0), 1.0, 0.0).astype(jnp.bfloat16)

    def combine(b, at):
        tiles, seens = [], []
        for d in range(devices):
            hop = lax.rem(me + devices - d, devices)
            far = jnp.maximum(hop - 1, 0)
            own = hop == 0
            tiles.append(jnp.where(own, stats[b], numbers[far, at]))
            seens.append(jnp.where(own, seen[b], parts[far, at]).astype(jnp.float32))
        top = functools.reduce(jnp.maximum, tiles)
        ratio = [jnp.exp2(x - top) for x in tiles]
        whole = functools.reduce(jnp.add, [pltpu.roll(x, 64, 1) * e for x, e in zip(tiles, ratio)])
        ratio = [e / whole for e in ratio]
        out = []
        for j in range(members):
            terms = [x[8 * j : 8 * j + 8] * jnp.broadcast_to(e[:, j : j + 1], (8, head)) for x, e in zip(seens, ratio)]
            out.append(functools.reduce(jnp.add, terms))
        mixed = jnp.concatenate(out, 0).astype(jnp.bfloat16)
        out_ref[b] = jnp.dot(unpick, mixed, preferred_element_type=jnp.float32).astype(jnp.bfloat16)

    def wait_recv(copies):
        for c in copies:
            c.wait_recv()

    def wait_send(copies):
        for c in copies:
            c.wait_send()

    def start(copies):
        for c in copies:
            c.start()

    def tick(t):
        @pl.when(t >= 1)
        def _():
            wait_send(group_sends(t - 1))

        @pl.when(t < groups)
        def _():
            start(group_sends(t))

        @pl.when(t >= 4)
        def _():
            wait_send(result_sends(t - 4))

        @pl.when(t >= 2)
        def _():
            start(result_sends(t - 2))

        @pl.when(t >= 1)
        def _():
            wait_recv(group_sends(t - 1))
            combine((t - 1) * devices + me, t - 1)

    acc_ref[...] = jnp.zeros_like(acc_ref)
    sums[...] = jnp.zeros_like(sums)

    fetch_k(0).wait()
    for b in range(1, SLOTS - 1):
        fetch_k(b + 1).start()
        fetch_v(b).start()
    body(0, None)

    def step(b):
        fetch_k(b + 1).wait()
        fetch_v(b).wait()

        @pl.when(b + SLOTS < batch)
        def _():
            fetch_k(b + SLOTS).start()

        @pl.when(b - 1 + SLOTS < last)
        def _():
            fetch_v(b - 1 + SLOTS).start()

        @pl.when(b - 1 + SLOTS == last)
        def _():
            for n in range(steps // GROUP):
                fetch_piece(n).start()

        finish(jnp.maximum(b - 1, 0))
        body(b + 1, b)

    def loop(b, _):
        step(b)

        @pl.when((b >= devices) & (lax.rem(b, devices) == 0))
        def _():
            tick(lax.div(b, devices) - 1)

        return 0

    lax.fori_loop(0, last - 2, loop, 0)
    fetch_k(last - 1).wait()
    finish(last - 3)
    body(last - 1, None)
    start(last_sends(0))
    fetch_v(last - 2).wait()
    body(None, last - 2)
    fetch_k(last).wait()
    finish(last - 2)
    body(last, None)
    start(last_sends(1))
    fetch_v(last - 1).wait()
    body(None, last - 1)
    finish(last - 1)
    start(last_sends(2))

    pieces = steps // GROUP

    def before(g):
        for n in range(pieces - 1) if g == 0 else [g] if g == pieces - 1 else []:
            fetch_piece(n).wait()

    body(None, last, before)
    finish_seen(last)
    start(last_sends(devices - 1)[0::2])
    finish_stats(last)
    start(last_sends(devices - 1)[1::2])
    tick(groups)
    wait_send(result_sends(groups - 3))
    start(result_sends(groups - 1))
    for n in range(devices):
        wait_recv(last_sends(n))
        combine(batch - devices + n, groups + n)
    for g in range(groups):
        wait_recv(result_sends(g))
    for g in range(groups - 2, groups):
        wait_send(result_sends(g))
    for n in range(devices):
        wait_send(last_sends(n))


def attend(mesh, q, k, v):
    batch, tokens, heads, head = k.shape
    devices = mesh.shape["sp"]
    queries = q.shape[1]
    rows = tokens * heads
    peers, groups, dma = devices - 1, batch // devices - 1, pltpu.SemaphoreType.DMA
    bf16, f32 = jnp.bfloat16, jnp.float32
    any_space = pl.BlockSpec(memory_space=pl.ANY)
    vmem = pl.BlockSpec(memory_space=pltpu.VMEM)
    return pl.pallas_call(
        functools.partial(kernel, devices, head**-0.5 * LOG2E),
        out_shape=pltpu.VMEM(q.shape, bf16),
        in_specs=[any_space] * 3,
        out_specs=vmem,
        scratch_shapes=[
            pltpu.VMEM(q.shape, bf16),
            pltpu.VMEM((SLOTS, rows, head), bf16),
            pltpu.VMEM((SLOTS, rows, head), bf16),
            pltpu.VMEM((2, 8, rows), f32),
            pltpu.VMEM((2, 8, 128), f32),
            pltpu.VMEM((queries, head), f32),
            pltpu.VMEM((2, 8, 128), f32),
            pltpu.VMEM((batch, queries, head), bf16),
            pltpu.VMEM((batch, queries, head), bf16),
            pltpu.VMEM((batch, 8, 128), f32),
            pltpu.VMEM((peers, groups + devices, queries, head), bf16),
            pltpu.VMEM((peers, groups + devices, 8, 128), f32),
            dma,
            dma((SLOTS,)),
            dma((SLOTS,)),
            dma((rows // (GROUP * ROWS),)),
            dma((peers,)),
            dma((peers,)),
            dma((peers, groups)),
            dma((peers, groups)),
            dma((peers, 2)),
            dma((peers, groups)),
            *[dma((peers, devices))] * 4,
        ],
        compiler_params=pltpu.CompilerParams(collective_id=0, has_side_effects=True, vmem_limit_bytes=60 * 2**20),
        cost_estimate=pl.CostEstimate(flops=8 * 4 * q.size * tokens, bytes_accessed=2 * 2 * k.size, transcendentals=q.shape[0] * queries * tokens),
    )(q, k.reshape(batch, rows, head), v.reshape(batch, rows, head))


def solution(mesh):
    return jax.shard_map(
        functools.partial(attend, mesh),
        mesh=mesh,
        in_specs=(P("dp", None, None), P("dp", "sp", None, None), P("dp", "sp", None, None)),
        out_specs=P("dp", None, None),
        check_vma=False,
    )
```
